256 devices in a mesh: dp: 16 (over x, z_lo), hyper: 16 (over y, z_hi, core).
Axes of the slice: x: 4, y: 4, z: 8 (z_hi: 2, z_lo: 4; z = z_hi * 4 + z_lo), core: 2. Of those that a mesh axis runs over, the one named last changes fastest.
Arguments:
- inputs: bfloat16 [512, 64, 128], P(('dp', 'hyper')), may hold values from -64 to 64
- labels: int32 [512, 64], P(('dp', 'hyper')), may hold values from 0 to 255
- client_ids: int32 [512], P(('dp', 'hyper')), may hold values from 0 to 511
- ext_weight: bfloat16 [128, 4096], replicated, may hold values from -0.5 to 0.5
- ext_bias: bfloat16 [4096], replicated, may hold values from -3 to 3
- embeddings: bfloat16 [512, 128], replicated, may hold values from -1.5 to 1.5
- hyper_in: bfloat16 [128, 50], replicated, may hold values from -2.09375 to 2.09375
- hyper_bias: float32 [50], replicated, may hold values from -3 to 3
- hyper_out: bfloat16 [4096, 50, 256], P('hyper'), may hold values from -0.1796875 to 0.1796875
Outputs:
- grad_ext_weight: float32 [128, 4096], replicated
- grad_ext_bias: float32 [4096], replicated
- grad_embeddings: float32 [512, 128], replicated
- grad_hyper_in: float32 [128, 50], replicated
- grad_hyper_bias: float32 [50], replicated
- grad_hyper_out: float32 [4096, 50, 256], P(('hyper', 'dp'))
The draws below stay inside these ranges and needn't reach their ends.
Inputs may be any that keep to these rules, and one draw needn't show every extreme that they name: `client_ids`: A client may hold several slots or none.
All inputs are finite; a program needn't handle non-finite values.
Results may differ from the reference program's by a relative error of at most 0.014.
The reference program's roundings to bfloat16 on the way count: a program that leaves them out, or rounds other values in their place, can miss the bound.
Values may be sent and summed in bfloat16 or wider, within the bound.
A program may use at most 128 MiB of HBM per device.

```python
import jax
import jax.numpy as jnp
from jax import lax

D = 4096
C = 256
DIN = 128
HH = 50
E = 128
CD = 2
R = 64
SLOTS = 512
NCL = 512
N_DP = 16
N_HYPER = 16


def draw_inputs(key, part):
    values = jax.random.normal(key, (SLOTS, R, DIN), jnp.float32)
    values = jnp.clip(values, -6.0, 6.0)
    return jnp.clip(values, -64.0, 64.0).astype(jnp.bfloat16)


def with_ends(result, key, low, high):
    shape = result.shape
    place = [jax.random.randint(jax.random.fold_in(key, axis), (), 0, shape[axis]) for axis in range(len(shape))]
    result = result.at[tuple(place)].set(low)
    longest = shape.index(max(shape))
    place[longest] = (place[longest] + 1) % shape[longest]
    return result.at[tuple(place)].set(high)


def block_scale(rng, dims, cuts, smallest, high):
    loudness = 1.0
    for axis_at, shards_of in cuts:
        draws = jax.random.uniform(jax.random.fold_in(jax.random.fold_in(rng, 6), axis_at), (shards_of,), jnp.float32, smallest / len(cuts), high / len(cuts))
        loudness = loudness * jnp.repeat(jnp.exp(draws), dims[axis_at] // shards_of).reshape((-1,) + (1,) * (len(dims) - 1 - axis_at))
    return loudness


def gaussian(own_key, extent, spread, bound, shards=(), kind=jnp.bfloat16):
    loudness = block_scale(own_key, extent, shards, -0.22, 0.18) if shards else 1.0
    array = jax.random.normal(own_key, extent, jnp.float32) * spread * loudness
    return jnp.minimum(jnp.maximum(array, -bound), bound).astype(kind)


def setup_inputs(seed: int = 0) -> dict:
    splits = jax.random.split(jax.random.key(seed), 10)
    return {
        "inputs": draw_inputs(jax.random.fold_in(splits[9], 71), 0),
        "labels": with_ends(jax.random.randint(splits[1], (SLOTS, R), 0, C), jax.random.fold_in(splits[1], 1), 0, C - 1).astype(jnp.int32),
        "client_ids": with_ends(jax.random.randint(splits[2], (SLOTS,), 0, NCL), jax.random.fold_in(splits[2], 1), 0, NCL - 1).astype(jnp.int32),
        "ext_weight": gaussian(splits[3], (DIN, D), DIN ** -0.5, 0.5),
        "ext_bias": gaussian(splits[4], (D,), 0.5, 3.0),
        "embeddings": gaussian(splits[5], (NCL, E), 0.25, 1.5),
        "hyper_in": gaussian(splits[6], (E, HH), 0.35, 2.09375),
        "hyper_bias": gaussian(splits[7], (HH,), 0.5, 3.0, (), jnp.float32),
        "hyper_out": gaussian(splits[8], (D, HH, C), 0.03, 0.1796875, ((0, 16),)),
    }


highest = lax.Precision.HIGHEST


def silu_slope(values):
    logistic = jax.nn.sigmoid(values)
    return logistic * (1.0 + values * (1.0 - logistic))


def class_grads(logits, slot_labels, row_count):
    largest = jnp.max(logits, axis=-1, keepdims=True)
    exponent = jnp.exp(logits - largest)
    probability = exponent / jnp.sum(exponent, axis=-1, keepdims=True)
    classes = jnp.arange(logits.shape[-1], dtype=jnp.int32)
    onehot = (slot_labels[..., None] == classes).astype(jnp.float32)
    return ((probability - onehot) / row_count).astype(jnp.bfloat16)


def reference(inputs, labels, client_ids, ext_weight, ext_bias, embeddings, hyper_in, hyper_bias, hyper_out):
    group_size = N_HYPER * CD
    hyper_wide = hyper_out.astype(jnp.float32)
    hyper_in_wide = hyper_in.astype(jnp.float32)
    client_table = jnp.arange(NCL, dtype=jnp.int32)

    def one_group(totals, group_index):
        first_slot = (group_index * group_size).astype(jnp.int32)
        slot_inputs = lax.dynamic_slice_in_dim(inputs, first_slot, group_size, 0)
        slot_labels = lax.dynamic_slice_in_dim(labels, first_slot, group_size, 0)
        slot_ids = lax.dynamic_slice_in_dim(client_ids, first_slot, group_size, 0)
        flat_in = slot_inputs.reshape(group_size * R, DIN)
        preact = jnp.dot(flat_in, ext_weight, preferred_element_type=jnp.float32) + ext_bias.astype(jnp.float32)
        features = jax.nn.silu(preact).astype(jnp.bfloat16).reshape(group_size, R, D)
        picked = embeddings[slot_ids]
        hyper_preact = jnp.dot(picked, hyper_in, preferred_element_type=jnp.float32) + hyper_bias
        hidden = jax.nn.silu(hyper_preact).astype(jnp.bfloat16)
        client_heads = jnp.einsum("kh,dhc->kdc", hidden.astype(jnp.float32), hyper_wide).astype(jnp.bfloat16)
        feat_wide = features.astype(jnp.float32)
        heads_wide = client_heads.astype(jnp.float32)
        logits = jnp.einsum("krd,kdc->krc", feat_wide, heads_wide)
        dlogits = class_grads(logits, slot_labels, R)
        dlog_wide = dlogits.astype(jnp.float32)
        dheads = jnp.einsum("krd,krc->kdc", feat_wide, dlog_wide).astype(jnp.bfloat16)
        dfeatures = jnp.einsum("krc,kdc->krd", dlog_wide, heads_wide).astype(jnp.bfloat16)
        dpreact = (dfeatures.reshape(group_size * R, D).astype(jnp.float32) * silu_slope(preact)).astype(jnp.bfloat16)
        grad_weight = jnp.dot(flat_in.T, dpreact, preferred_element_type=jnp.float32)
        grad_bias = jnp.sum(dpreact.astype(jnp.float32), axis=0)
        dheads_wide = dheads.astype(jnp.float32)
        group_out = jnp.einsum("kh,kdc->dhc", hidden.astype(jnp.float32), dheads_wide)
        group_out = lax.optimization_barrier(group_out.astype(jnp.bfloat16)).astype(jnp.float32)
        dhidden = jnp.einsum("kdc,dhc->kh", dheads_wide, hyper_wide)
        hyper_dpre = dhidden * silu_slope(hyper_preact)
        grad_in = jnp.dot(picked.astype(jnp.float32).T, hyper_dpre, precision=highest)
        grad_hbias = jnp.sum(hyper_dpre, axis=0)
        select = (slot_ids[:, None] == client_table[None, :]).astype(jnp.float32)
        grad_table = jnp.dot(select.T, jnp.dot(hyper_dpre, hyper_in_wide.T, precision=highest), precision=highest)
        updated = (totals[0] + grad_weight, totals[1] + grad_bias, totals[2] + grad_table,
                   totals[3] + grad_in, totals[4] + grad_hbias, totals[5] + group_out)
        return updated, None

    initial = (jnp.zeros((DIN, D), jnp.float32), jnp.zeros((D,), jnp.float32), jnp.zeros((NCL, E), jnp.float32),
               jnp.zeros((E, HH), jnp.float32), jnp.zeros((HH,), jnp.float32), jnp.zeros((D, HH, C), jnp.float32))
    totals, unused = lax.scan(one_group, initial, jnp.arange(N_DP, dtype=jnp.int32))
    return (totals[0], totals[1], totals[2], totals[3], totals[4], totals[5])
```

```python
import functools

import jax
import jax.numpy as jnp
from jax import lax
from jax.experimental import pallas as pl
from jax.experimental.pallas import tpu as pltpu
from jax.sharding import Mesh
from jax.sharding import PartitionSpec as P

AXES = ("x", "zl", "y", "zh", "core")
SIZES = (4, 4, 4, 2, 2)
HYPER = ("y", "zh", "core")
NDP = 16
PIECES = 4
MESH = pl.DeviceIdType.MESH
VMEM = pltpu.VMEM
F32 = jnp.float32
BF16 = jnp.bfloat16


def remote(src, dst, send, recv, device):
    return pltpu.make_async_remote_copy(
        src_ref=src, dst_ref=dst, send_sem=send, recv_sem=recv, device_id=device, device_id_type=MESH
    )


def hyper_place():
    y, zh, core = lax.axis_index("y"), lax.axis_index("zh"), lax.axis_index("core")
    y_peers = [{"y": lax.rem(y + o, 4)} for o in (1, 2, 3)]
    return y, zh, core, y_peers, {"zh": 1 - zh}, {"core": 1 - core}


def greet(devices):
    barrier = pltpu.get_barrier_semaphore()
    for device in devices:
        pl.semaphore_signal(barrier, inc=1, device_id=device, device_id_type=MESH)
    pl.semaphore_wait(barrier, len(devices))


class Gather:
    def __init__(self, buf, send, recv):
        self.buf, self.send, self.recv = buf, send, recv
        self.y, self.zh, self.core, self.y_peers, self.z_peer, self.c_peer = hyper_place()
        self.copies = {}

    def push(self, index, y, zh, device):
        block = self.buf.at[y, zh, self.core]
        copy = remote(block, block, self.send.at[index], self.recv.at[index], device)
        copy.start()
        self.copies[index] = copy

    def first(self):
        self.push(0, self.y, self.zh, self.z_peer)
        for i, peer in enumerate(self.y_peers):
            self.push(1 + i, self.y, self.zh, peer)
        self.push(7, self.y, self.zh, self.c_peer)

    def second(self):
        other = 1 - self.zh
        self.copies[0].wait_recv()
        for i, peer in enumerate(self.y_peers):
            self.push(4 + i, self.y, other, peer)
        self.push(8, self.y, other, self.c_peer)

    def third(self):
        for i in range(3):
            self.copies[1 + i].wait_recv()
            self.push(9 + i, lax.rem(self.y + 3 - i, 4), self.zh, self.c_peer)

    def fourth(self):
        for i in range(3):
            self.copies[4 + i].wait_recv()
            self.push(12 + i, lax.rem(self.y + 3 - i, 4), 1 - self.zh, self.c_peer)

    def last(self):
        for i in range(7, 15):
            self.copies[i].wait_recv()
        for i in range(15):
            self.copies[i].wait_send()


def gather_kernel(x_ref, ids_ref, x_out, ids_out, sx, rx, si, ri):
    y, zh, core, y_peers, z_peer, c_peer = hyper_place()
    ids_out[y, zh, core] = ids_ref[...]
    x_out[y, zh, core] = x_ref[...]
    greet([*y_peers, z_peer, c_peer])
    gathers = (Gather(ids_out, si, ri), Gather(x_out, sx, rx))
    for step in ("first", "second", "third", "fourth", "last"):
        for gather in gathers:
            getattr(gather, step)()


def logits_kernel(part, labels, out, r1, r2, r3, s2, c_send, c_recv, y_send, y_recv, z_send, z_recv, g_send, g_recv):
    y, zh, core, y_peers, z_peer, c_peer = hyper_place()
    greet([*y_peers, z_peer, c_peer])
    planes = (1 - zh, zh)
    copies = []
    for q, plane in enumerate(planes):
        copy = remote(part.at[:, plane, 1 - core], r1.at[plane], c_send.at[q], c_recv.at[q], c_peer)
        copy.start()
        copies.append(copy)
    y_copies = {}
    for q, plane in enumerate(planes):
        copies[q].wait_recv()
        for i, peer in enumerate(y_peers):
            to = lax.rem(y + 1 + i, 4)
            r1[plane, to] = r1[plane, to] + part[to, plane, core]
            copy = remote(r1.at[plane, to], r2.at[q, i], y_send.at[q, i], y_recv.at[q, i], peer)
            copy.start()
            y_copies[q, i] = copy
    total = r1[planes[0], y] + part[y, planes[0], core]
    for i in range(3):
        y_copies[0, i].wait_recv()
        total = total + r2[0, i]
    s2[...] = total
    z_copy = remote(s2, r3, z_send, z_recv, z_peer)
    z_copy.start()
    logits = r1[zh, y] + part[y, zh, core]
    for i in range(3):
        y_copies[1, i].wait_recv()
        logits = logits + r2[1, i]
    z_copy.wait_recv()
    logits = logits + r3[...]
    largest = jnp.max(logits, axis=-1, keepdims=True)
    exponent = jnp.exp(logits - largest)
    probability = exponent / jnp.sum(exponent, axis=-1, keepdims=True)
    classes = lax.broadcasted_iota(jnp.int32, logits.shape, 2)
    onehot = (labels[...] == classes).astype(F32)
    out[y, zh, core] = ((probability - onehot) / logits.shape[1]).astype(BF16)
    gather = Gather(out, g_send, g_recv)
    for step in ("first", "second", "third", "fourth", "last"):
        getattr(gather, step)()
    for copy in [*copies, *y_copies.values(), z_copy]:
        copy.wait_send()


def tail_kernel(
    g, e, gb, dhid, slope, ident, out, ew, gbh, hd,
    r1, rs, rd, tz, rz, re, gball, ha, hy, hz, hc,
    x1_s, x1_r, xs_s, xs_r, xd_s, xd_r, zz_s, zz_r,
    e_s, e_r, ea_s, ea_r, b_s, b_r, h_s, h_r, hx_s, hx_r, gw_s, gw_r, gg_s, gg_r,
):
    y, zh, core, y_peers, z_peer, c_peer = hyper_place()
    x, zl = lax.axis_index("x"), lax.axis_index("zl")
    dp = x * 4 + zl
    right, left = lax.rem(x + 1, 4), lax.rem(x + 3, 4)
    far = lax.rem(x + 2, 4)
    to_right, to_left = {"x": right}, {"x": left}

    def dp_device(o):
        to = lax.rem(dp + o, NDP)
        return to, {"x": to // 4, "zl": to % 4}

    greet([*y_peers, z_peer, c_peer, *[dp_device(o)[1] for o in range(1, NDP)]])

    c_copy = remote(dhid, hc, hx_s.at[0], hx_r.at[0], c_peer)
    c_copy.start()
    gball[dp] = gb[...]
    e_copies, b_copies = [], []
    for o in range(1, NDP):
        to, device = dp_device(o)
        copy = remote(e.at[to], re.at[o - 1], e_s.at[o - 1], e_r.at[o - 1], device)
        copy.start()
        e_copies.append(copy)
        copy = remote(gb, gball.at[dp], b_s.at[o - 1], b_r.at[o - 1], device)
        copy.start()
        b_copies.append(copy)

    rows = g.shape[2] // (2 * PIECES)
    cut = [pl.ds(p * rows, rows) for p in range(2 * PIECES)]
    far_copies, sum_copies, own_copies = {}, {}, {}
    order = [p for j in range(PIECES) for p in (j, PIECES + j)]
    for p in order:
        device = to_right if p < PIECES else to_left
        copy = remote(g.at[far, :, cut[p]], r1.at[p], x1_s.at[p], x1_r.at[p], device)
        copy.start()
        far_copies[p] = copy

    c_copy.wait_recv()
    ha[...] = dhid[...] + hc[...]
    hy_copies = []
    for i, peer in enumerate(y_peers):
        copy = remote(ha, hy.at[i], hx_s.at[1 + i], hx_r.at[1 + i], peer)
        copy.start()
        hy_copies.append(copy)
    partial = ha[...]
    for i in range(3):
        hy_copies[i].wait_recv()
        partial = partial + hy[i]
    hz[0] = partial
    hz_copy = remote(hz.at[0], hz.at[1], hx_s.at[4], hx_r.at[4], z_peer)
    hz_copy.start()

    total = e[dp]
    for o in range(1, NDP):
        e_copies[o - 1].wait_recv()
        total = total + re[o - 1]
    ew[y, zh, core, dp] = total.astype(BF16)
    ea_copies = []
    own_rows = ew.at[y, zh, core, dp]
    for o in range(1, NDP):
        copy = remote(own_rows, own_rows, ea_s.at[o - 1], ea_r.at[o - 1], dp_device(o)[1])
        copy.start()
        ea_copies.append(copy)
    bias = gb[...]
    for o in range(1, NDP):
        b_copies[o - 1].wait_recv()
    for i in range(1, NDP):
        bias = bias + gball[lax.rem(dp + i, NDP)]
    gbh[y, zh, core] = bias
    gb_gather = Gather(gbh, gg_s, gg_r)
    gb_gather.first()
    hz_copy.wait_recv()
    hd[dp] = (hz[0] + hz[1]) * slope[...] + ident[...]
    h_copies = []
    for o in range(1, NDP):
        copy = remote(hd.at[dp], hd.at[dp], h_s.at[o - 1], h_r.at[o - 1], dp_device(o)[1])
        copy.start()
        h_copies.append(copy)
    gb_gather.second()

    def passed_on(p):
        far_copies[p].wait_recv()
        if p < PIECES:
            chunk, device, back, other = right, to_right, left, to_left
        else:
            chunk, device, back, other = left, to_left, right, to_right
        r1[p] = (r1[p].astype(F32) + g[chunk, :, cut[p]].astype(F32)).astype(BF16)
        copy = remote(r1.at[p], rs.at[p], xs_s.at[p], xs_r.at[p], device)
        copy.start()
        sum_copies[p] = copy
        copy = remote(g.at[back, :, cut[p]], rd.at[p], xd_s.at[p], xd_r.at[p], other)
        copy.start()
        own_copies[p] = copy

    z_copies = {}

    def spread(p):
        sum_copies[p].wait_recv()
        own_copies[p].wait_recv()
        tz[p] = (g[x, :, cut[p]].astype(F32) + rs[p].astype(F32) + rd[p].astype(F32)).astype(BF16)
        for i in range(3):
            to = lax.rem(zl + 1 + i, 4)
            copy = remote(tz.at[p, to], rz.at[i, p], zz_s.at[i, p], zz_r.at[i, p], {"zl": to})
            copy.start()
            z_copies[i, p] = copy

    for p in order:
        passed_on(p)
    gw_gather = Gather(ew, gw_s, gw_r)
    gb_gather.third()
    gb_gather.fourth()
    for copy in ea_copies:
        copy.wait_recv()
    gw_gather.first()
    half = len(order) // 2
    for p in order[:half]:
        spread(p)
    gw_gather.second()
    for p in order[half:]:
        spread(p)
    gw_gather.third()
    gw_gather.fourth()
    for p in order:
        value = tz[p, zl].astype(F32)
        for i in range(3):
            z_copies[i, p].wait_recv()
            value = value + rz[i, p].astype(F32)
        out[cut[p]] = value

    for copy in h_copies:
        copy.wait_recv()
    gb_gather.last()
    gw_gather.last()
    sent = [c_copy, *e_copies, *b_copies, *far_copies.values(), *hy_copies, hz_copy, *ea_copies, *h_copies]
    for copy in [*sent, *sum_copies.values(), *own_copies.values(), *z_copies.values()]:
        copy.wait_send()


def call(kernel, outs, scratch, ident, args, limit, flops):
    size = sum(a.size * a.dtype.itemsize for a in [*args, *outs])
    return pl.pallas_call(
        kernel,
        out_shape=outs,
        in_specs=[pl.BlockSpec(memory_space=VMEM)] * len(args),
        out_specs=[pl.BlockSpec(memory_space=VMEM)] * len(outs),
        scratch_shapes=scratch,
        compiler_params=pltpu.CompilerParams(
            collective_id=ident, has_side_effects=True, vmem_limit_bytes=limit
        ),
        cost_estimate=pl.CostEstimate(flops=flops, bytes_accessed=size, transcendentals=0),
    )(*args)


def dma(*shape):
    return pltpu.SemaphoreType.DMA(shape)


def shape_of(shape, dtype):
    return jax.ShapeDtypeStruct(shape, dtype)


def gather_inputs(inputs, ids):
    outs = [shape_of((4, 2, 2, *inputs.shape), BF16), shape_of((4, 2, 2, *ids.shape), jnp.int32)]
    return call(gather_kernel, outs, [dma(15), dma(15), dma(15), dma(15)], 0, (inputs, ids), 16 << 20, 10**9)


def exchange_logits(part, labels):
    block = part.shape[3:]
    scratch = [
        VMEM((2, 4, *block), F32),
        VMEM((2, 3, *block), F32),
        VMEM(block, F32),
        VMEM(block, F32),
        dma(2), dma(2), dma(2, 3), dma(2, 3), pltpu.SemaphoreType.DMA, pltpu.SemaphoreType.DMA, dma(15), dma(15),
    ]
    outs = [shape_of((4, 2, 2, *block), BF16)]
    return call(logits_kernel, outs, scratch, 1, (part, labels), 32 << 20, 10**9)[0]


def tail(g, e, gb, dhid, slope, ident):
    rows, hh, cc = g.shape[2:]
    pieces = 2 * PIECES
    piece = (pieces, 4, rows // pieces, hh, cc)
    n = NDP - 1
    scratch = [
        VMEM(piece, BF16), VMEM(piece, BF16), VMEM(piece, BF16), VMEM(piece, BF16),
        VMEM((3, pieces, *piece[2:]), BF16),
        VMEM((n, *e.shape[1:]), F32),
        VMEM((NDP, *gb.shape), F32),
        VMEM(dhid.shape, F32), VMEM((3, *dhid.shape), F32), VMEM((2, *dhid.shape), F32), VMEM(dhid.shape, F32),
        dma(pieces), dma(pieces), dma(pieces), dma(pieces), dma(pieces), dma(pieces), dma(3, pieces), dma(3, pieces),
        dma(n), dma(n), dma(n), dma(n), dma(n), dma(n), dma(n), dma(n), dma(5), dma(5), dma(15), dma(15), dma(15), dma(15),
    ]
    outs = [
        shape_of((rows, hh, cc), F32),
        shape_of((4, 2, 2, *e.shape), BF16),
        shape_of((4, 2, 2, *gb.shape), F32),
        shape_of((NDP, *dhid.shape), F32),
    ]
    return call(tail_kernel, outs, scratch, 2, (g, e, gb, dhid, slope, ident), 48 << 20, 10**9)


def silu_slope(values):
    logistic = jax.nn.sigmoid(values)
    return logistic * (1.0 + values * (1.0 - logistic))


def pick(ids, embeddings):
    table_ids = jnp.arange(embeddings.shape[0], dtype=jnp.int32)
    select = (ids[:, None] == table_ids[None, :]).astype(BF16)
    return select, jnp.dot(select, embeddings, preferred_element_type=F32).astype(BF16)


def local(
    inputs, labels, client_ids, ext_weight, ext_bias, embeddings, hyper_in, hyper_bias, hyper_out
):
    own_slots, row_count, width_in = inputs.shape
    cols, hh, classes = hyper_out.shape
    slots = own_slots * 16
    hyper = lax.axis_index(HYPER)

    ids_tile = jnp.pad(client_ids[None, :], ((0, 7), (0, 128 - own_slots)))
    in_all, ids_all = gather_inputs(inputs, ids_tile)
    flat_in = in_all.reshape(slots * row_count, width_in)
    ids = ids_all[:, :, :, 0, :own_slots].reshape(slots)

    _, picked = pick(ids, embeddings)
    hyper_preact = jnp.dot(picked, hyper_in, preferred_element_type=F32) + hyper_bias
    hidden = jax.nn.silu(hyper_preact).astype(BF16)
    heads = jnp.einsum("kh,dhc->kdc", hidden, hyper_out, preferred_element_type=F32).astype(BF16)

    weight = lax.dynamic_slice_in_dim(ext_weight, hyper * cols, cols, 1)
    bias = lax.dynamic_slice_in_dim(ext_bias, hyper * cols, cols, 0)
    preact = jnp.dot(flat_in, weight, preferred_element_type=F32) + bias.astype(F32)
    features = jax.nn.silu(preact).astype(BF16).reshape(slots, row_count, cols)

    part = jnp.einsum("krd,kdc->krc", features, heads, preferred_element_type=F32)
    part = part.reshape(4, 2, 2, own_slots, row_count, classes)
    dlogits = exchange_logits(part, labels[:, :, None]).reshape(slots, row_count, classes)

    dheads = jnp.einsum("krd,krc->kdc", features, dlogits, preferred_element_type=F32).astype(BF16)
    dfeatures = jnp.einsum("krc,kdc->krd", dlogits, heads, preferred_element_type=F32).astype(BF16)
    dpreact = (dfeatures.reshape(slots * row_count, cols).astype(F32) * silu_slope(preact)).astype(BF16)
    grad_weight = jnp.dot(flat_in.T, dpreact, preferred_element_type=F32)
    grad_bias = jnp.sum(dpreact.astype(F32), axis=0)
    grad_out = jnp.einsum("kh,kdc->dhc", hidden, dheads, preferred_element_type=F32).astype(BF16)
    dhidden = jnp.einsum("kdc,dhc->kh", dheads, hyper_out, preferred_element_type=F32)

    lanes = ((0, 0), (0, 128 - hh))
    slope = jnp.pad(silu_slope(hyper_preact), lanes)
    ident = jnp.zeros((slots, 128), F32).at[:, 64].set(ids.astype(F32))
    grad_out, grad_weight, grad_bias, spread = tail(
        grad_out.reshape(4, 4, cols // NDP, hh, classes),
        grad_weight.reshape(NDP, width_in // NDP, cols),
        jnp.pad(grad_bias.reshape(cols // 128, 128), ((0, 8 - cols // 128), (0, 0))),
        jnp.pad(dhidden, lanes),
        slope,
        ident,
    )
    grad_weight = grad_weight.reshape(16, width_in, cols).transpose(1, 0, 2).reshape(width_in, 16 * cols).astype(F32)
    grad_bias = grad_bias[:, :, :, : cols // 128].reshape(16 * cols)

    spread = spread.reshape(NDP * slots, 128)
    every_id = spread[:, 64].astype(jnp.int32)
    hyper_dpre = spread[:, :hh]
    select, every_picked = pick(every_id, embeddings)
    highest = lax.Precision.HIGHEST
    grad_in = jnp.dot(every_picked.astype(F32).T, hyper_dpre, precision=highest)
    grad_hbias = jnp.sum(hyper_dpre, axis=0)
    back = jnp.dot(hyper_dpre, hyper_in.astype(F32).T, precision=highest)
    grad_table = jnp.dot(select.astype(F32).T, back, precision=highest)
    return grad_weight, grad_bias, grad_table, grad_in, grad_hbias, grad_out


def solution(mesh):
    torus = Mesh(mesh.devices.reshape(SIZES), AXES)
    placed = (P(AXES, None, None), P(AXES, None), P(AXES), P(), P(), P(), P(), P(), P(HYPER, None, None))
    return jax.shard_map(
        local,
        mesh=torus,
        in_specs=placed,
        out_specs=(P(), P(), P(), P(), P(), P((*HYPER, "x", "zl"), None, None)),
        check_vma=False,
    )
```

```python
import functools

import jax
import jax.numpy as jnp
from jax import lax
from jax.experimental import pallas as pl
from jax.experimental.pallas import tpu as pltpu
from jax.sharding import Mesh
from jax.sharding import PartitionSpec as P

AXES = ("x", "zl", "y", "zh", "core")
SIZES = (4, 4, 4, 2, 2)
HYPER = ("y", "zh", "core")
NDP = 16
HH = 50
HP = 64
MESH = pl.DeviceIdType.MESH
VMEM = pltpu.VMEM
F32 = jnp.float32
BF16 = jnp.bfloat16


def remote(src, dst, send, recv, device):
    return pltpu.make_async_remote_copy(
        src_ref=src, dst_ref=dst, send_sem=send, recv_sem=recv, device_id=device, device_id_type=MESH
    )


def hyper_place():
    y, zh, core = lax.axis_index("y"), lax.axis_index("zh"), lax.axis_index("core")
    y_peers = [{"y": lax.rem(y + o, 4)} for o in (1, 2, 3)]
    return y, zh, core, y_peers, {"zh": 1 - zh}, {"core": 1 - core}


def greet(devices):
    barrier = pltpu.get_barrier_semaphore()
    for device in devices:
        pl.semaphore_signal(barrier, inc=1, device_id=device, device_id_type=MESH)
    pl.semaphore_wait(barrier, len(devices))


class Gather:
    def __init__(self, buf, send, recv):
        self.buf, self.send, self.recv = buf, send, recv
        self.y, self.zh, self.core, self.y_peers, self.z_peer, self.c_peer = hyper_place()
        self.copies = {}

    def push(self, index, y, zh, device):
        block = self.buf.at[y, zh, self.core]
        copy = remote(block, block, self.send.at[index], self.recv.at[index], device)
        copy.start()
        self.copies[index] = copy

    def first(self):
        self.push(0, self.y, self.zh, self.z_peer)
        for i, peer in enumerate(self.y_peers):
            self.push(1 + i, self.y, self.zh, peer)
        self.push(7, self.y, self.zh, self.c_peer)

    def second(self):
        other = 1 - self.zh
        self.copies[0].wait_recv()
        for i, peer in enumerate(self.y_peers):
            self.push(4 + i, self.y, other, peer)
        self.push(8, self.y, other, self.c_peer)

    def third(self):
        for i in range(3):
            self.copies[1 + i].wait_recv()
            self.push(9 + i, lax.rem(self.y + 3 - i, 4), self.zh, self.c_peer)

    def fourth(self):
        for i in range(3):
            self.copies[4 + i].wait_recv()
            self.push(12 + i, lax.rem(self.y + 3 - i, 4), 1 - self.zh, self.c_peer)

    def last(self):
        for i in range(7, 15):
            self.copies[i].wait_recv()
        for i in range(15):
            self.copies[i].wait_send()


def gather_kernel(x_ref, ids_ref, x_out, ids_out, sx, rx, si, ri):
    y, zh, core, y_peers, z_peer, c_peer = hyper_place()
    ids_out[y, zh, core] = ids_ref[...]
    x_out[y, zh, core] = x_ref[...]
    greet([*y_peers, z_peer, c_peer])
    gathers = (Gather(ids_out, si, ri), Gather(x_out, sx, rx))
    for step in ("first", "second", "third", "fourth", "last"):
        for gather in gathers:
            getattr(gather, step)()


def logits_kernel(part, labels, out, r1, r2, r3, s2, c_send, c_recv, y_send, y_recv, z_send, z_recv, g_send, g_recv):
    y, zh, core, y_peers, z_peer, c_peer = hyper_place()
    greet([*y_peers, z_peer, c_peer])
    planes = (1 - zh, zh)
    copies = []
    for q, plane in enumerate(planes):
        copy = remote(part.at[:, plane, 1 - core], r1.at[plane], c_send.at[q], c_recv.at[q], c_peer)
        copy.start()
        copies.append(copy)
    y_copies = {}
    for q, plane in enumerate(planes):
        copies[q].wait_recv()
        for i, peer in enumerate(y_peers):
            to = lax.rem(y + 1 + i, 4)
            r1[plane, to] = r1[plane, to] + part[to, plane, core]
            copy = remote(r1.at[plane, to], r2.at[q, i], y_send.at[q, i], y_recv.at[q, i], peer)
            copy.start()
            y_copies[q, i] = copy
    total = r1[planes[0], y] + part[y, planes[0], core]
    for i in range(3):
        y_copies[0, i].wait_recv()
        total = total + r2[0, i]
    s2[...] = total
    z_copy = remote(s2, r3, z_send, z_recv, z_peer)
    z_copy.start()
    logits = r1[zh, y] + part[y, zh, core]
    for i in range(3):
        y_copies[1, i].wait_recv()
        logits = logits + r2[1, i]
    z_copy.wait_recv()
    logits = logits + r3[...]
    largest = jnp.max(logits, axis=-1, keepdims=True)
    exponent = jnp.exp(logits - largest)
    probability = exponent / jnp.sum(exponent, axis=-1, keepdims=True)
    classes = lax.broadcasted_iota(jnp.int32, logits.shape, 2)
    onehot = (labels[...] == classes).astype(F32)
    out[y, zh, core] = ((probability - onehot) / logits.shape[1]).astype(BF16)
    gather = Gather(out, g_send, g_recv)
    for step in ("first", "second", "third", "fourth", "last"):
        getattr(gather, step)()
    for copy in [*copies, *y_copies.values(), z_copy]:
        copy.wait_send()


def iota(shape, dim):
    return lax.broadcasted_iota(jnp.int32, shape, dim)


def onehot(mask, dtype=BF16):
    return jnp.where(mask, jnp.ones(mask.shape, F32), jnp.zeros(mask.shape, F32)).astype(dtype)


def dot(a, b, dims, precision=None):
    return lax.dot_general(a, b, ((dims[:1], dims[1:]), ((), ())), precision=precision, preferred_element_type=F32)


def tail_kernel(
    feat, dl, heads, slope, flat_in, w, hid, hslope, ident, emb, hin,
    out, gw_out, gb_out, table_out, gin_out, ghb_out,
    dh, block, acc, g, r1, rs, rd, tz, rz, e, re, gb, gball, ew, gbh, hd, dhid, ha, hy, hz, hc,
    x1_s, x1_r, xs_s, xs_r, xd_s, xd_r, zz_s, zz_r,
    e_s, e_r, ea_s, ea_r, b_s, b_r, h_s, h_r, hx_s, hx_r, gw_s, gw_r, gg_s, gg_r,
):
    y, zh, core, y_peers, z_peer, c_peer = hyper_place()
    x, zl = lax.axis_index("x"), lax.axis_index("zl")
    dp = x * 4 + zl
    right, left, far = lax.rem(x + 1, 4), lax.rem(x + 3, 4), lax.rem(x + 2, 4)
    toward = ({"x": right}, {"x": left})
    slots, row_count, cols = feat.shape
    classes = dl.shape[2]
    hh, hp = HH, HP

    def dp_device(o):
        to = lax.rem(dp + o, NDP)
        return to, {"x": to // 4, "zl": to % 4}

    greet([*y_peers, z_peer, c_peer, *[dp_device(o)[1] for o in range(1, NDP)]])

    row, col = iota((8 * hh, hp), 0), iota((8 * hh, hp), 1)
    group = sum((row >= hh * j).astype(jnp.int32) for j in range(1, 8))
    spread_h = onehot(row - hh * group == col)
    by_slot = dot(spread_h, hid[...], (1, 1)).astype(BF16)
    row, col = iota((slots, 8 * slots), 0), iota((slots, 8 * slots), 1)
    spread_k = onehot(row == (col >> 3))
    full = dot(by_slot, spread_k, (1, 0))
    row, col = iota(full.shape, 0), iota(full.shape, 1)
    group = sum((row >= hh * j).astype(jnp.int32) for j in range(1, 8))
    block[...] = jnp.where(group == (col & 7), full, jnp.zeros_like(full)).astype(BF16)

    def one_slot(k, carry):
        dh[k] = dot(feat[k], dl[k], (0, 0)).astype(BF16).astype(F32)
        return carry

    lax.fori_loop(0, slots, one_slot, 0)

    def rows_of(d0):
        return dh[:, pl.ds(pl.multiple_of(d0, 8), 8), :].reshape(8 * slots, classes).astype(BF16)

    z_target = [lax.rem(zl + o, 4) for o in (2, 1, 3, 0)]

    def z_of(q):
        if isinstance(q, int):
            return z_target[q]
        return jnp.where(q == 0, z_target[0], jnp.where(q == 1, z_target[1], jnp.where(q == 2, z_target[2], z_target[3])))

    def piece(chunk, q, half):
        zt = z_of(q)
        x8 = rows_of((chunk * 4 + zt) * 16 + half * 8)
        g[chunk, zt, half] = jnp.dot(block[...], x8, preferred_element_type=F32).astype(BF16)

    def far_copy(half, q):
        return remote(g.at[far, z_of(q), half], r1.at[half, q], x1_s.at[half, q], x1_r.at[half, q], toward[half])

    def own_copy(half, q):
        chunk = left if half == 0 else right
        return remote(g.at[chunk, z_of(q), half], rd.at[half, q], xd_s.at[half, q], xd_r.at[half, q], toward[1 - half])

    def sum_copy(half, q):
        return remote(r1.at[half, q], rs.at[half, q], xs_s.at[half, q], xs_r.at[half, q], toward[half])

    def z_copy(half, q):
        return remote(tz.at[half, q], rz.at[half, q], zz_s.at[half, q], zz_r.at[half, q], {"zl": z_of(q)})

    def both(make, q):
        for half in range(2):
            make(half, q).start()

    def passed_on(q):
        for half in range(2):
            far_copy(half, q).wait_recv()
            chunk = right if half == 0 else left
            r1[half, q] = (r1[half, q].astype(F32) + g[chunk, z_of(q), half].astype(F32)).astype(BF16)
            sum_copy(half, q).start()

    def spread(q):
        for half in range(2):
            sum_copy(half, q).wait_recv()
            own_copy(half, q).wait_recv()
            total = g[x, z_of(q), half].astype(F32) + rs[half, q].astype(F32) + rd[half, q].astype(F32)
            tz[half, q] = total.astype(BF16)
            if q < 3:
                z_copy(half, q).start()

    def pieces(chunks, q):
        for chunk in chunks:
            for half in range(2):
                piece(chunk, q, half)

    for q in range(2):
        pieces((far,), q)
        both(far_copy, q)

    e[...] = jnp.zeros_like(e)
    gb[...] = jnp.zeros_like(gb)

    def four_slots(i, carry):
        parts = []
        for j in range(4):
            k = i * 4 + j
            dfeat = dot(dl[k], heads[k], (1, 1)).astype(BF16).astype(F32)
            parts.append((dfeat * slope[k]).astype(BF16))
        dpre = jnp.concatenate(parts, axis=0)
        here = flat_in[pl.ds(pl.multiple_of(i * 4 * row_count, 4 * row_count), 4 * row_count), :]
        e[...] += dot(here, dpre, (0, 0)).reshape(e.shape)
        gb[...] += jnp.sum(dpre.astype(F32), axis=0, keepdims=True)
        return carry

    lax.fori_loop(0, slots // 4, four_slots, 0)
    gball[dp] = gb[...]
    e_copies, b_copies = [], []
    for o in range(1, NDP):
        to, device = dp_device(o)
        copy = remote(e.at[to], re.at[o - 1], e_s.at[o - 1], e_r.at[o - 1], device)
        copy.start()
        e_copies.append(copy)
        copy = remote(gb, gball.at[dp], b_s.at[o - 1], b_r.at[o - 1], device)
        copy.start()
        b_copies.append(copy)

    def rest(q, carry):
        pieces((right, left), q)
        return carry

    lax.fori_loop(0, 4, rest, 0)
    both(own_copy, 0)
    for q in (2, 3):
        pieces((far,), q)
    passed_on(0)
    both(far_copy, 2)
    both(own_copy, 1)

    def own_pieces(q, carry):
        pieces((x,), q)
        return carry

    lax.fori_loop(0, 4, own_pieces, 0)

    acc[...] = jnp.zeros_like(acc)
    gap = jnp.zeros((8, hp - hh, classes), BF16)

    def two_groups(i, carry):
        value = acc[...]
        for j in range(2):
            d0 = (i * 2 + j) * 8
            w8 = jnp.concatenate([w[pl.ds(d0, 8)], gap], axis=1).reshape(8 * hp, classes)
            value = value + dot(rows_of(d0), w8, (1, 1))
        acc[...] = value
        return carry

    lax.fori_loop(0, cols // 16, two_groups, 0)
    highest = lax.Precision.HIGHEST
    row, col = iota(acc.shape, 0), iota(acc.shape, 1)
    kept = jnp.where((row & 7) == (col >> 6), acc[...], jnp.zeros_like(acc[...]))
    by_k = dot(onehot(iota((slots, 8 * slots), 0) == (iota((slots, 8 * slots), 1) >> 3), F32), kept, (1, 0), highest)
    fold = onehot((iota((8 * hp, 128), 0) & (hp - 1)) == iota((8 * hp, 128), 1), F32)
    dhid[...] = dot(by_k, fold, (1, 0), highest)
    c_copy = remote(dhid, hc, hx_s.at[0], hx_r.at[0], c_peer)
    c_copy.start()

    passed_on(1)
    both(far_copy, 3)
    both(own_copy, 2)

    c_copy.wait_recv()
    ha[...] = dhid[...] + hc[...]
    hy_copies = []
    for i, peer in enumerate(y_peers):
        copy = remote(ha, hy.at[i], hx_s.at[1 + i], hx_r.at[1 + i], peer)
        copy.start()
        hy_copies.append(copy)

    total = e[dp]
    for o in range(1, NDP):
        e_copies[o - 1].wait_recv()
        total = total + re[o - 1]
    ew[y, zh, core, dp] = total.astype(BF16)
    own_rows = ew.at[y, zh, core, dp]
    ea_copies = []
    for o in range(1, NDP):
        copy = remote(own_rows, own_rows, ea_s.at[o - 1], ea_r.at[o - 1], dp_device(o)[1])
        copy.start()
        ea_copies.append(copy)
    bias = gb[...]
    for o in range(1, NDP):
        b_copies[o - 1].wait_recv()
        bias = bias + gball[lax.rem(dp + NDP - o, NDP)]
    gbh[y, zh, core] = bias
    gb_gather = Gather(gbh, gg_s, gg_r)
    gb_gather.first()

    partial = ha[...]
    for i in range(3):
        hy_copies[i].wait_recv()
        partial = partial + hy[i]
    hz[0] = partial
    hz_copy = remote(hz.at[0], hz.at[1], hx_s.at[4], hx_r.at[4], z_peer)
    hz_copy.start()
    gb_gather.second()

    spread(0)
    passed_on(2)
    both(own_copy, 3)

    hz_copy.wait_recv()
    hd[dp] = (hz[0] + hz[1]) * hslope[...] + ident[...]
    h_copies = []
    for o in range(1, NDP):
        copy = remote(hd.at[dp], hd.at[dp], h_s.at[o - 1], h_r.at[o - 1], dp_device(o)[1])
        copy.start()
        h_copies.append(copy)
    gb_gather.third()
    gb_gather.fourth()
    for copy in ea_copies:
        copy.wait_recv()
    gw_gather = Gather(ew, gw_s, gw_r)
    gw_gather.first()

    spread(1)
    passed_on(3)
    gw_gather.second()
    gw_gather.third()

    for copy in h_copies:
        copy.wait_recv()
    every = hd[...].reshape(NDP * slots, 128)
    lane = iota(every.shape, 1)
    hyper_dpre = jnp.where(lane < hh, every, jnp.zeros_like(every))
    clients = emb.shape[0]
    same = iota((NDP * slots, clients), 1).astype(F32) == every[:, 64:65]
    select = onehot(same, F32)
    picked = dot(select.astype(BF16), emb[...], (1, 0))
    gin_out[...] = dot(picked, hyper_dpre, (0, 0), highest)
    ghb_out[...] = jnp.sum(hyper_dpre, axis=0, keepdims=True)
    back = dot(hyper_dpre, hin[...].astype(F32), (1, 1), highest)
    table_out[...] = dot(select, back, (0, 0), highest)

    spread(2)
    gw_gather.fourth()
    spread(3)
    gb_gather.last()
    for i in range(16):
        at = (i // 4, (i // 2) % 2, i % 2)
        gb_out[:, i * cols : (i + 1) * cols] = gbh[at]
    gw_gather.last()
    for i in range(16):
        at = (i // 4, (i // 2) % 2, i % 2)
        gw_out[:, i * cols : (i + 1) * cols] = ew[at].astype(F32).reshape(-1, cols)
    for half in range(2):
        value = tz[half, 3].astype(F32)
        for q in range(3):
            z_copy(half, q).wait_recv()
            value = value + rz[half, q].astype(F32)
        for j in range(8):
            out[half * 8 + j] = value[j * hh : (j + 1) * hh]

    for half in range(2):
        for q in range(4):
            for make in (far_copy, own_copy, sum_copy):
                make(half, q).wait_send()
            if q < 3:
                z_copy(half, q).wait_send()
    for copy in [c_copy, *e_copies, *b_copies, *hy_copies, hz_copy, *ea_copies, *h_copies]:
        copy.wait_send()


def call(kernel, outs, scratch, ident, args, limit, flops):
    size = sum(a.size * a.dtype.itemsize for a in [*args, *outs])
    return pl.pallas_call(
        kernel,
        out_shape=outs,
        in_specs=[pl.BlockSpec(memory_space=VMEM)] * len(args),
        out_specs=[pl.BlockSpec(memory_space=VMEM)] * len(outs),
        scratch_shapes=scratch,
        compiler_params=pltpu.CompilerParams(
            collective_id=ident, has_side_effects=True, vmem_limit_bytes=limit
        ),
        cost_estimate=pl.CostEstimate(flops=flops, bytes_accessed=size, transcendentals=0),
    )(*args)


def dma(*shape):
    return pltpu.SemaphoreType.DMA(shape)


def shape_of(shape, dtype):
    return jax.ShapeDtypeStruct(shape, dtype)


def gather_inputs(inputs, ids):
    outs = [shape_of((4, 2, 2, *inputs.shape), BF16), shape_of((4, 2, 2, *ids.shape), jnp.int32)]
    return call(gather_kernel, outs, [dma(15), dma(15), dma(15), dma(15)], 0, (inputs, ids), 16 << 20, 10**9)


def exchange_logits(part, labels):
    block = part.shape[3:]
    scratch = [
        VMEM((2, 4, *block), F32),
        VMEM((2, 3, *block), F32),
        VMEM(block, F32),
        VMEM(block, F32),
        dma(2), dma(2), dma(2, 3), dma(2, 3), pltpu.SemaphoreType.DMA, pltpu.SemaphoreType.DMA, dma(15), dma(15),
    ]
    outs = [shape_of((4, 2, 2, *block), BF16)]
    return call(logits_kernel, outs, scratch, 1, (part, labels), 32 << 20, 10**9)[0]


def tail(feat, dl, heads, slope, flat_in, w, hid, hslope, ident, emb, hin):
    slots, row_count, cols = feat.shape
    classes = dl.shape[2]
    width_in = flat_in.shape[1]
    piece = (8 * HH, classes)
    n = NDP - 1
    rows = (NDP, width_in // NDP, cols)
    lanes = hslope.shape
    scratch = [
        VMEM((slots, cols, classes), F32),
        VMEM((8 * HH, 8 * slots), BF16),
        VMEM((8 * slots, 8 * HP), F32),
        VMEM((4, 4, 2, *piece), BF16),
        VMEM((2, 4, *piece), BF16), VMEM((2, 4, *piece), BF16), VMEM((2, 4, *piece), BF16), VMEM((2, 4, *piece), BF16),
        VMEM((2, 3, *piece), BF16),
        VMEM(rows, F32), VMEM((n, *rows[1:]), F32),
        VMEM((1, cols), F32), VMEM((NDP, 1, cols), F32),
        VMEM((4, 2, 2, *rows), BF16), VMEM((4, 2, 2, 1, cols), F32),
        VMEM((NDP, *lanes), F32),
        VMEM(lanes, F32), VMEM(lanes, F32), VMEM((3, *lanes), F32), VMEM((2, *lanes), F32), VMEM(lanes, F32),
        dma(2, 4), dma(2, 4), dma(2, 4), dma(2, 4), dma(2, 4), dma(2, 4), dma(2, 3), dma(2, 3),
        dma(n), dma(n), dma(n), dma(n), dma(n), dma(n), dma(n), dma(n), dma(5), dma(5), dma(15), dma(15), dma(15), dma(15),
    ]
    outs = [
        shape_of((16, HH, classes), F32),
        shape_of((width_in, 16 * cols), F32),
        shape_of((1, 16 * cols), F32),
        shape_of(emb.shape, F32),
        shape_of((emb.shape[1], 128), F32),
        shape_of((1, 128), F32),
    ]
    args = (feat, dl, heads, slope, flat_in, w, hid, hslope, ident, emb, hin)
    return call(tail_kernel, outs, scratch, 2, args, 64000 << 10, 10**10)


def silu_slope(values):
    logistic = jax.nn.sigmoid(values)
    return logistic * (1.0 + values * (1.0 - logistic))


def pick(ids, embeddings):
    table_ids = jnp.arange(embeddings.shape[0], dtype=jnp.int32)
    select = (ids[:, None] == table_ids[None, :]).astype(BF16)
    return select, jnp.dot(select, embeddings, preferred_element_type=F32).astype(BF16)


def local(
    inputs, labels, client_ids, ext_weight, ext_bias, embeddings, hyper_in, hyper_bias, hyper_out
):
    own_slots, row_count, width_in = inputs.shape
    cols, hh, classes = hyper_out.shape
    slots = own_slots * 16
    hyper = lax.axis_index(HYPER)

    ids_tile = jnp.pad(client_ids[None, :], ((0, 7), (0, 128 - own_slots)))
    in_all, ids_all = gather_inputs(inputs, ids_tile)
    flat_in = in_all.reshape(slots * row_count, width_in)
    ids = ids_all[:, :, :, 0, :own_slots].reshape(slots)

    _, picked = pick(ids, embeddings)
    hyper_preact = jnp.dot(picked, hyper_in, preferred_element_type=F32) + hyper_bias
    hidden = jax.nn.silu(hyper_preact).astype(BF16)
    heads = jnp.einsum("kh,dhc->kdc", hidden, hyper_out, preferred_element_type=F32).astype(BF16)

    weight = lax.dynamic_slice_in_dim(ext_weight, hyper * cols, cols, 1)
    bias = lax.dynamic_slice_in_dim(ext_bias, hyper * cols, cols, 0)
    preact = jnp.dot(flat_in, weight, preferred_element_type=F32) + bias.astype(F32)
    features = jax.nn.silu(preact).astype(BF16).reshape(slots, row_count, cols)

    part = jnp.einsum("krd,kdc->krc", features, heads, preferred_element_type=F32)
    part = part.reshape(4, 2, 2, own_slots, row_count, classes)
    dlogits = exchange_logits(part, labels[:, :, None]).reshape(slots, row_count, classes)

    lanes = ((0, 0), (0, 128 - hh))
    hslope = jnp.pad(silu_slope(hyper_preact), lanes)
    ident = jnp.zeros((slots, 128), F32).at[:, 64].set(ids.astype(F32))
    grad_out, grad_weight, grad_bias, grad_table, grad_in, grad_hbias = tail(
        features,
        dlogits,
        heads,
        silu_slope(preact).reshape(features.shape),
        flat_in,
        hyper_out,
        jnp.pad(hidden, ((0, 0), (0, HP - hh))),
        hslope,
        ident,
        embeddings,
        jnp.pad(hyper_in, lanes),
    )
    return grad_weight, grad_bias[0], grad_table, grad_in[:, :hh], grad_hbias[0, :hh], grad_out


def solution(mesh):
    torus = Mesh(mesh.devices.reshape(SIZES), AXES)
    placed = (P(AXES, None, None), P(AXES, None), P(AXES), P(), P(), P(), P(), P(), P(HYPER, None, None))
    return jax.shard_map(
        local,
        mesh=torus,
        in_specs=placed,
        out_specs=(P(), P(), P(), P(), P(), P((*HYPER, "x", "zl"), None, None)),
        check_vma=False,
    )
```
